16 devices in a mesh: dp: 2 (over y, z), cp: 8 (over x, core).
Axes of the slice: x: 4, y: 2, z: 1, core: 2. Of those that a mesh axis runs over, the one named last changes fastest.
The devices are a block of a 4x4x8 slice.
Arguments:
- x: bfloat16 [4096, 4096], P(('dp', 'cp')), parts along dimension 0
- k_cache: bfloat16 [32768, 8, 128], P(('dp', 'cp')), parts along dimension 0
- v_cache: bfloat16 [32768, 8, 128], P(('dp', 'cp')), parts along dimension 0
- ln_gain: bfloat16 [4096], replicated
- w_q: bfloat16 [4096, 4096], replicated
- w_k: bfloat16 [4096, 1024], replicated
- w_v: bfloat16 [4096, 1024], replicated
- w_o: bfloat16 [4096, 4096], replicated
- q_gain: bfloat16 [128], replicated
- k_gain: bfloat16 [128], replicated
Outputs:
- output 1: bfloat16 [4096, 4096], P(('dp', 'cp')), parts along dimension 0
- output 2: bfloat16 [4096, 8, 128], P(('dp', 'cp')), parts along dimension 0
- output 3: bfloat16 [4096, 8, 128], P(('dp', 'cp')), parts along dimension 0
There are 2 independent parts. The reference program is written for one: setup_inputs(seed, part) draws one part's arguments, and reference() takes and returns one part's arrays. A program takes and returns all parts, laid end to end along the dimension named above; an argument that names none is the same for every part.
All inputs are finite; a program needn't handle non-finite values.
Results may differ from the reference program's by a relative error of at most 0.0118422.
Values are sent between devices in bfloat16 or wider.
A program may use at most 768 MiB of HBM per device.

```python
import jax
import jax.numpy as jnp
from jax import lax

HIDDEN = 4096
Q_HEADS = 32
KV_HEADS = 8
HEAD_DIM = 128
NEW_LEN = 2048
PREFIX_LEN = 16384
ROW_BLOCK = 16
ROPE_THETA = 1.0e6
NORM_EPS = 1.0e-6


def setup_inputs(seed: int = 0, part: int = 0) -> dict:
    part_key = jax.random.fold_in(jax.random.key(seed), part)
    part_keys = jax.random.split(part_key, 3)
    shared = jax.random.split(jax.random.key(seed + 1), 7)
    q_width = Q_HEADS * HEAD_DIM
    kv_width = KV_HEADS * HEAD_DIM
    total_len = PREFIX_LEN + NEW_LEN
    x = jax.random.normal(part_keys[0], (NEW_LEN, HIDDEN), jnp.float32)
    k_cache = jax.random.normal(part_keys[1], (PREFIX_LEN, KV_HEADS, HEAD_DIM), jnp.float32)
    v_cache = jax.random.normal(part_keys[2], (PREFIX_LEN, KV_HEADS, HEAD_DIM), jnp.float32)
    ln_gain = 1.0 + 0.4 * jax.random.normal(shared[0], (HIDDEN,), jnp.float32)
    w_q = jax.random.normal(shared[1], (HIDDEN, q_width), jnp.float32) * HIDDEN ** -0.5
    w_k = jax.random.normal(shared[2], (HIDDEN, kv_width), jnp.float32) * HIDDEN ** -0.5
    w_v = jax.random.normal(shared[3], (HIDDEN, kv_width), jnp.float32) * HIDDEN ** -0.5
    w_o = jax.random.normal(shared[4], (q_width, HIDDEN), jnp.float32) * (0.5 * (total_len / q_width) ** 0.5)
    q_gain = 1.0 + 0.3 * jax.random.normal(shared[5], (HEAD_DIM,), jnp.float32)
    k_gain = 1.5 + 0.3 * jax.random.normal(shared[6], (HEAD_DIM,), jnp.float32)
    return {'x': x.astype(jnp.bfloat16), 'k_cache': k_cache.astype(jnp.bfloat16), 'v_cache': v_cache.astype(jnp.bfloat16), 'ln_gain': ln_gain.astype(jnp.bfloat16), 'w_q': w_q.astype(jnp.bfloat16), 'w_k': w_k.astype(jnp.bfloat16), 'w_v': w_v.astype(jnp.bfloat16), 'w_o': w_o.astype(jnp.bfloat16), 'q_gain': q_gain.astype(jnp.bfloat16), 'k_gain': k_gain.astype(jnp.bfloat16)}


def rms_norm(vals, gain):
    mean_sq = jnp.mean(vals * vals, axis=-1, keepdims=True)
    return vals * lax.rsqrt(mean_sq + NORM_EPS) * gain


def apply_rope(vals, positions):
    half = HEAD_DIM // 2
    inv_freq = ROPE_THETA ** (-jnp.arange(half, dtype=jnp.float32) * (2.0 / HEAD_DIM))
    angles = positions.astype(jnp.float32)[:, None] * inv_freq[None, :]
    cos_tab = jnp.cos(angles)[:, None, :]
    sin_tab = jnp.sin(angles)[:, None, :]
    first = vals[..., :half]
    second = vals[..., half:]
    return jnp.concatenate([first * cos_tab - second * sin_tab, second * cos_tab + first * sin_tab], axis=-1)


def reference(x, k_cache, v_cache, ln_gain, w_q, w_k, w_v, w_o, q_gain, k_gain):
    group = Q_HEADS // KV_HEADS
    scale = HEAD_DIM ** -0.5
    x_wide = x.astype(jnp.float32)
    hidden = rms_norm(x_wide, ln_gain.astype(jnp.float32)).astype(jnp.bfloat16)
    q_raw = jnp.dot(hidden, w_q, preferred_element_type=jnp.float32).astype(jnp.bfloat16)
    k_raw = jnp.dot(hidden, w_k, preferred_element_type=jnp.float32).astype(jnp.bfloat16)
    v_new = jnp.dot(hidden, w_v, preferred_element_type=jnp.float32).astype(jnp.bfloat16).reshape(NEW_LEN, KV_HEADS, HEAD_DIM)
    positions = PREFIX_LEN + jnp.arange(NEW_LEN)
    q_rot = apply_rope(rms_norm(q_raw.reshape(NEW_LEN, Q_HEADS, HEAD_DIM).astype(jnp.float32), q_gain.astype(jnp.float32)), positions).astype(jnp.bfloat16)
    k_new = apply_rope(rms_norm(k_raw.reshape(NEW_LEN, KV_HEADS, HEAD_DIM).astype(jnp.float32), k_gain.astype(jnp.float32)), positions).astype(jnp.bfloat16)
    keys_all = jnp.concatenate([k_cache, k_new], axis=0).astype(jnp.float32)
    values_all = jnp.concatenate([v_cache, v_new], axis=0).astype(jnp.float32)
    key_pos = jnp.arange(PREFIX_LEN + NEW_LEN)
    block_count = NEW_LEN // ROW_BLOCK
    q_blocks = q_rot.reshape(block_count, ROW_BLOCK, KV_HEADS, group, HEAD_DIM)

    def block_attend(block):
        q_block, block_index = block
        row_pos = PREFIX_LEN + block_index * ROW_BLOCK + jnp.arange(ROW_BLOCK)
        scores = jnp.einsum('rkgd,skd->rkgs', q_block.astype(jnp.float32), keys_all) * scale
        allowed = key_pos[None, :] <= row_pos[:, None]
        scores = jnp.where(allowed[:, None, None, :], scores, -jnp.inf)
        peak = jnp.max(scores, axis=-1, keepdims=True)
        weights = jnp.exp(scores - peak)
        probs = weights / jnp.sum(weights, axis=-1, keepdims=True)
        return jnp.einsum('rkgs,skd->rkgd', probs, values_all)

    attended = lax.map(block_attend, (q_blocks, jnp.arange(block_count)))
    attended = attended.reshape(NEW_LEN, Q_HEADS * HEAD_DIM).astype(jnp.bfloat16)
    out = (x_wide + jnp.dot(attended, w_o, preferred_element_type=jnp.float32)).astype(jnp.bfloat16)
    return (out, k_new, v_new)
```

```python
import functools

import jax
import jax.numpy as jnp
from jax import lax
from jax.experimental import pallas as pl
from jax.experimental.pallas import tpu as pltpu
from jax.sharding import PartitionSpec as P

HEAD_DIM = 128
ROPE_THETA = 1.0e6
NORM_EPS = 1.0e-6
SCALE2 = HEAD_DIM ** -0.5 * 1.4426950408889634
KEY_BLOCK = 256
NEW_UNIT = 4
W_SLOTS = 4
W_COLS = 512
MESH = pl.DeviceIdType.MESH
NEG_INF = float('-inf')


def rope_tables(positions):
    half = HEAD_DIM // 2
    inv_freq = ROPE_THETA ** (-jnp.arange(half, dtype=jnp.float32) * (2.0 / HEAD_DIM))
    angles = positions.astype(jnp.float32)[:, None] * inv_freq[None, :]
    cos_tab = jnp.cos(angles)
    sin_tab = jnp.sin(angles)
    return jnp.concatenate([cos_tab, cos_tab], axis=-1), jnp.concatenate([-sin_tab, sin_tab], axis=-1)


def ring_order(n):
    chips = n // 2
    order = [(0, 0), (0, 1)]
    for d in range(1, chips // 2 + 1):
        if 2 * d == chips:
            order += [(d, 0), (d, 1)]
        else:
            order += [(d, 0), (chips - d, 0), (d, 1), (chips - d, 1)]
    return order


def make_kernel(n, rows, cache_rows, group):
    order = ring_order(n)
    chips = n // 2
    qcols = group * HEAD_DIM
    tile_q = 512
    halves = rows * group // tile_q
    tiles = n * halves
    phases = n // 2
    blocks = 2 * cache_rows // KEY_BLOCK
    per_chunk = cache_rows // KEY_BLOCK
    kv_per_tile = W_COLS // HEAD_DIM

    def kernel(x_ref, gain_ref, qg_ref, kg_ref, cos_ref, sin_ref, kc, vc, wq, wk, wv, wo,
               out_ref, kn_ref, vn_ref,
               h_ref, wbuf, kbuf, vbuf, qsend, qbuf, nkbuf, nvsend, nvbuf, osend, obuf,
               s_ref, s2_ref, acc, m_ref, l_ref, mx_ref,
               wsem, lsem, sk, rk, sv, rv, sq, rq, snk, rnk, snv, rnv, so, ro):
        me = lax.axis_index('cp')
        chip = me // 2
        core = me % 2

        def peer(j):
            if isinstance(j, int):
                dc, fl = order[j]
            else:
                dc, fl = jnp.int32(0), jnp.int32(0)
                for i, (a, b) in enumerate(order):
                    dc = jnp.where(j == i, a, dc)
                    fl = jnp.where(j == i, b, fl)
            return ((chip + dc) % chips) * 2 + (core + fl) % 2

        def remote(src, dst, ssem, rsem, dev):
            return pltpu.make_async_remote_copy(src_ref=src, dst_ref=dst, send_sem=ssem, recv_sem=rsem,
                                                device_id={'cp': dev}, device_id_type=MESH)

        def k_copy(dev, who):
            return remote(kc.at[dev], kbuf.at[who], sk.at[dev], rk.at[who], dev)

        def v_copy(dev, who):
            return remote(vc.at[dev], vbuf.at[who], sv.at[dev], rv.at[who], dev)

        def q_copy(dev, who):
            return remote(qsend.at[dev], qbuf.at[who], sq.at[dev], rq.at[who], dev)

        def nk_copy(dev, who):
            return remote(kn_ref.at[dev], nkbuf.at[who], snk.at[dev], rnk.at[who], dev)

        def nv_copy(dev, who):
            return remote(nvsend.at[dev], nvbuf.at[who], snv.at[dev], rnv.at[who], dev)

        def o_copy(dev, who):
            return remote(osend.at[dev], obuf.at[who], so.at[dev], ro.at[who], dev)

        def w_copy(src, col, slot):
            return pltpu.make_async_copy(src.at[:, pl.ds(pl.multiple_of(col * W_COLS, W_COLS), W_COLS)],
                                         wbuf.at[slot], wsem.at[slot])

        def q_dest(t):
            if isinstance(t, int):
                return peer(t + 2 if t < n - 2 else n - 1 - t)
            return peer(jnp.where(t < n - 2, t + 2, n - 1 - t))

        for t in range(W_SLOTS):
            w_copy(wq, q_dest(t), t).start()
        own_k = pltpu.make_async_copy(kc.at[me], kbuf.at[me], lsem.at[0])
        own_v = pltpu.make_async_copy(vc.at[me], vbuf.at[me], lsem.at[1])
        own_k.start()
        own_v.start()

        barrier = pltpu.get_barrier_semaphore()
        for j in range(1, n):
            pl.semaphore_signal(barrier, inc=1, device_id={'cp': peer(j)}, device_id_type=MESH)
        pl.semaphore_wait(barrier, n - 1)

        early = [1, 2, 3]
        late = [j for j in range(1, n) if j not in early]
        for j in early:
            k_copy(peer(j), me).start()
            v_copy(peer(j), me).start()

        gain = gain_ref[...].astype(jnp.float32)

        def norm_rows(r, _):
            sl = pl.ds(pl.multiple_of(r * 16, 16), 16)
            xw = x_ref[sl, :].astype(jnp.float32)
            ms = jnp.mean(xw * xw, axis=-1, keepdims=True)
            h_ref[sl, :] = (xw * lax.rsqrt(ms + NORM_EPS) * gain).astype(jnp.bfloat16)
            return 0

        lax.fori_loop(0, rows // 16, norm_rows, 0)

        def init_tile(t, _):
            acc[t] = jnp.zeros((HEAD_DIM, tile_q), jnp.float32)
            m_ref[t] = jnp.full((8, tile_q), NEG_INF, jnp.float32)
            l_ref[t] = jnp.zeros((8, tile_q), jnp.float32)
            return 0

        lax.fori_loop(0, tiles, init_tile, 0)

        def project(slot):
            return jnp.dot(h_ref[...], wbuf[slot], preferred_element_type=jnp.float32).astype(jnp.bfloat16)

        def norm_rope(raw, head_gain):
            val = raw.astype(jnp.float32)
            ms = jnp.mean(val * val, axis=-1, keepdims=True)
            val = val * lax.rsqrt(ms + NORM_EPS) * head_gain
            return (val * cos_ref[...] + pltpu.roll(val, HEAD_DIM // 2, 1) * sin_ref[...]).astype(jnp.bfloat16)

        q_gain = qg_ref[...].astype(jnp.float32)
        k_gain = kg_ref[...].astype(jnp.float32)
        k_tiles = n // kv_per_tile

        def q_tile(t, _):
            slot = t % W_SLOTS
            dest = q_dest(t)
            w_copy(wq, dest, slot).wait()
            y = project(slot)
            for g in range(group):
                qsend[dest, pl.ds(g * rows, rows), :] = norm_rope(y[:, g * HEAD_DIM:(g + 1) * HEAD_DIM], q_gain)

            @pl.when(t < n - W_SLOTS)
            def _():
                w_copy(wq, q_dest(t + W_SLOTS), slot).start()

            for i in range(k_tiles):
                @pl.when(t == n - W_SLOTS + i)
                def _(i=i):
                    w_copy(wk, i, slot).start()

                @pl.when(t == n - W_SLOTS + k_tiles + i)
                def _(i=i):
                    w_copy(wv, i, slot).start()

            @pl.when(t < n - 1)
            def _():
                q_copy(dest, me).start()

            return 0

        lax.fori_loop(0, n, q_tile, 0)
        qbuf[me] = qsend[me]

        def k_tile(t, _):
            slot = (n + t) % W_SLOTS
            w_copy(wk, t, slot).wait()
            y = project(slot)
            for g in range(kv_per_tile):
                kn_ref[t * kv_per_tile + g] = norm_rope(y[:, g * HEAD_DIM:(g + 1) * HEAD_DIM], k_gain)
            w_copy(wo, t, slot).start()
            return 0

        lax.fori_loop(0, k_tiles, k_tile, 0)
        nkbuf[me] = kn_ref[me]

        def v_tile(t, _):
            slot = (n + k_tiles + t) % W_SLOTS
            w_copy(wv, t, slot).wait()
            y = project(slot)
            for g in range(kv_per_tile):
                val = y[:, g * HEAD_DIM:(g + 1) * HEAD_DIM]
                vn_ref[t * kv_per_tile + g] = val
                nvsend[t * kv_per_tile + g] = val.T
            w_copy(wo, k_tiles + t, slot).start()
            return 0

        lax.fori_loop(0, k_tiles, v_tile, 0)
        nvbuf[me] = nvsend[me]

        for j in late[:2]:
            k_copy(peer(j), me).start()
            v_copy(peer(j), me).start()
        for j in range(1, n):
            nk_copy(peer(j), me).start()
            nv_copy(peer(j), me).start()
        for j in late[2:]:
            k_copy(peer(j), me).start()
            v_copy(peer(j), me).start()

        def block_index(p, t):
            i = t // halves
            return jnp.where(p == phases - 1, n - 1 - i, i)

        def q_of(src, hf):
            return qbuf[src, pl.ds(pl.multiple_of(hf * tile_q, tile_q), tile_q), :]

        def qk(b, chunks, q):
            kk = kbuf[chunks[b // per_chunk], (b % per_chunk) * KEY_BLOCK:(b % per_chunk + 1) * KEY_BLOCK, :]
            s = lax.dot_general(kk, q, (((1,), (1,)), ((), ())), preferred_element_type=jnp.float32)
            s_ref[b * KEY_BLOCK:(b + 1) * KEY_BLOCK, :] = s
            return jnp.max(s.reshape(KEY_BLOCK // 8, 8, tile_q), axis=0)

        def fold(total, term, op):
            return term if total is None else op(total, term)

        def step(slot, chunks, next_chunks, next_q):
            m_old = m_ref[slot]
            m_new = jnp.maximum(m_old, jnp.max(mx_ref[...], axis=0, keepdims=True) * SCALE2)
            alpha = jnp.exp2(m_old - m_new)
            m_ref[slot] = m_new
            m_row = m_new[0:1]
            mx = ls = pv = None
            for b in range(blocks):
                p = jnp.exp2(s_ref[b * KEY_BLOCK:(b + 1) * KEY_BLOCK, :] * SCALE2 - m_row)
                ls = fold(ls, jnp.sum(p.reshape(KEY_BLOCK // 8, 8, tile_q), axis=0), jnp.add)
                mx = fold(mx, qk(b, next_chunks, next_q), jnp.maximum)
                vv = vbuf[chunks[b // per_chunk], :, (b % per_chunk) * KEY_BLOCK:(b % per_chunk + 1) * KEY_BLOCK]
                pv = fold(pv, jnp.dot(vv, p.astype(jnp.bfloat16), preferred_element_type=jnp.float32), jnp.add)
            mx_ref[...] = mx
            l_ref[slot] = l_ref[slot] * alpha + ls
            acc[slot] = acc[slot] * alpha[0:1] + pv

        def where_is(g):
            p = g // tiles
            t = g % tiles
            src = peer(block_index(p, t))
            hf = t % halves
            return p, t, src, hf

        def run(g, last):
            p, t, src, hf = where_is(g)
            g2 = jnp.minimum(g + 1, phases * tiles - 1)
            p2, t2, src2, hf2 = where_is(g2)

            if not last:
                @pl.when(jnp.logical_and(t2 == 0, p2 > 0))
                def _():
                    for c in range(2):
                        who = peer(2 * p2 + c)
                        k_copy(who, who).wait_recv()
                        v_copy(who, who).wait_recv()

                @pl.when(jnp.logical_and(p2 == 0, hf2 == 0))
                def _():
                    q_copy(src2, src2).wait_recv()

            step(src * halves + hf, [peer(2 * p), peer(2 * p + 1)], [peer(2 * p2), peer(2 * p2 + 1)], q_of(src2, hf2))
            return src, hf

        own_k.wait()
        own_v.wait()
        who = peer(1)
        k_copy(who, who).wait_recv()
        v_copy(who, who).wait_recv()
        first_q = q_of(me, 0)
        mx = None
        for b in range(blocks):
            mx = fold(mx, qk(b, [me, who], first_q), jnp.maximum)
        mx_ref[...] = mx

        def early_step(g, _):
            run(g, False)
            return 0

        lax.fori_loop(0, (phases - 1) * tiles, early_step, 0)

        for j in range(1, n):
            who = peer(j)
            nk_copy(who, who).wait_recv()
            nv_copy(who, who).wait_recv()

        def new_unit(src, hf, unit):
            slot = src * halves + hf
            q = q_of(src, hf)
            lane = lax.broadcasted_iota(jnp.int32, (KEY_BLOCK, tile_q), 1)
            diff = lane % rows - lax.broadcasted_iota(jnp.int32, (KEY_BLOCK, tile_q), 0)
            mx = None
            for b in range(NEW_UNIT):
                kb = unit * NEW_UNIT + b
                s = lax.dot_general(nkbuf[kb], q, (((1,), (1,)), ((), ())), preferred_element_type=jnp.float32)
                s = jnp.where(diff >= (kb - src) * rows, s, NEG_INF)
                s2_ref[b * KEY_BLOCK:(b + 1) * KEY_BLOCK, :] = s
                mx = fold(mx, jnp.max(s.reshape(KEY_BLOCK // 8, 8, tile_q), axis=0), jnp.maximum)
            m_old = m_ref[slot]
            m_new = jnp.maximum(m_old, jnp.max(mx, axis=0, keepdims=True) * SCALE2)
            alpha = jnp.exp2(m_old - m_new)
            m_ref[slot] = m_new
            m_row = m_new[0:1]
            ls = pv = None
            for b in range(NEW_UNIT):
                p = jnp.exp2(s2_ref[b * KEY_BLOCK:(b + 1) * KEY_BLOCK, :] * SCALE2 - m_row)
                ls = fold(ls, jnp.sum(p.reshape(KEY_BLOCK // 8, 8, tile_q), axis=0), jnp.add)
                pv = fold(pv, jnp.dot(nvbuf[unit * NEW_UNIT + b], p.astype(jnp.bfloat16), preferred_element_type=jnp.float32), jnp.add)
            l_ref[slot] = l_ref[slot] * alpha + ls
            acc[slot] = acc[slot] * alpha[0:1] + pv

        for unit in range(n // NEW_UNIT):
            def unit_step(i, _, unit=unit):
                t = i + unit * NEW_UNIT * halves
                new_unit(t // halves, t % halves, unit)
                return 0

            lax.fori_loop(0, (n - unit * NEW_UNIT) * halves, unit_step, 0)

        def late_step(g, _):
            src, hf = run(g, True)
            slot = src * halves + hf
            o = acc[slot] / jnp.sum(l_ref[slot], axis=0, keepdims=True)
            o = o.T.astype(jnp.bfloat16)
            for i in range(tile_q // rows):
                osend[src, hf * (tile_q // rows) + i] = o[i * rows:(i + 1) * rows]

            @pl.when(jnp.logical_and(hf == halves - 1, g < phases * tiles - 1))
            def _():
                o_copy(src, me).start()

            return 0

        lax.fori_loop((phases - 1) * tiles, phases * tiles, late_step, 0)
        obuf[me] = osend[me]

        for j in range(n - 1, 0, -1):
            who = peer(j)
            o_copy(who, who).wait_recv()
        o_all = jnp.concatenate([obuf[i, g] for i in range(n) for g in range(group)], axis=-1)
        h_ref[...] = o_all
        n_out = n

        def out_tile(t, _):
            slot = t % W_SLOTS
            w_copy(wo, t, slot).wait()
            y = jnp.dot(h_ref[...], wbuf[slot], preferred_element_type=jnp.float32)
            cols = pl.ds(pl.multiple_of(t * W_COLS, W_COLS), W_COLS)
            out_ref[:, cols] = (x_ref[:, cols].astype(jnp.float32) + y).astype(jnp.bfloat16)

            @pl.when(t < n_out - W_SLOTS)
            def _():
                w_copy(wo, t + W_SLOTS, slot).start()

            return 0

        lax.fori_loop(0, n_out, out_tile, 0)

        for j in range(1, n):
            who = peer(j)
            for copy in (k_copy, v_copy, q_copy, nk_copy, nv_copy, o_copy):
                copy(who, me).wait_send()

    return kernel


def solution(mesh):
    n = mesh.shape['cp']
    row_spec = P(('dp', 'cp'), None)
    cache_spec = P(('dp', 'cp'), None, None)
    whole = P()

    def device_step(x_rows, k_cache, v_cache, ln_gain, w_q, w_k, w_v, w_o, q_gain, k_gain):
        rows, hidden = x_rows.shape
        cache_rows, kv_heads, _ = k_cache.shape
        group = w_q.shape[1] // HEAD_DIM // kv_heads
        q_rows = rows * group
        tile_q = 512
        tiles = n * q_rows // tile_q
        positions = cache_rows * n + lax.axis_index('cp') * rows + jnp.arange(rows)
        cos_tab, sin_tab = rope_tables(positions)
        k_heads = jnp.transpose(k_cache, (1, 0, 2))
        v_heads = jnp.transpose(v_cache, (1, 2, 0))
        bf16 = jnp.bfloat16
        f32 = jnp.float32
        vmem = pl.BlockSpec(memory_space=pltpu.VMEM)
        hbm = pl.BlockSpec(memory_space=pl.ANY)
        dma = pltpu.SemaphoreType.DMA
        call = pl.pallas_call(
            make_kernel(n, rows, cache_rows, group),
            out_shape=(jax.ShapeDtypeStruct((rows, hidden), bf16),
                       jax.ShapeDtypeStruct((kv_heads, rows, HEAD_DIM), bf16),
                       jax.ShapeDtypeStruct((kv_heads, rows, HEAD_DIM), bf16)),
            in_specs=[vmem] * 6 + [hbm] * 6,
            out_specs=[vmem] * 3,
            scratch_shapes=[
                pltpu.VMEM((rows, hidden), bf16),
                pltpu.VMEM((W_SLOTS, hidden, W_COLS), bf16),
                pltpu.VMEM((n, cache_rows, HEAD_DIM), bf16),
                pltpu.VMEM((n, HEAD_DIM, cache_rows), bf16),
                pltpu.VMEM((n, q_rows, HEAD_DIM), bf16),
                pltpu.VMEM((n, q_rows, HEAD_DIM), bf16),
                pltpu.VMEM((n, rows, HEAD_DIM), bf16),
                pltpu.VMEM((n, HEAD_DIM, rows), bf16),
                pltpu.VMEM((n, HEAD_DIM, rows), bf16),
                pltpu.VMEM((n, group, rows, HEAD_DIM), bf16),
                pltpu.VMEM((n, group, rows, HEAD_DIM), bf16),
                pltpu.VMEM((2 * cache_rows, tile_q), f32),
                pltpu.VMEM((NEW_UNIT * KEY_BLOCK, tile_q), f32),
                pltpu.VMEM((tiles, HEAD_DIM, tile_q), f32),
                pltpu.VMEM((tiles, 8, tile_q), f32),
                pltpu.VMEM((tiles, 8, tile_q), f32),
                pltpu.VMEM((8, tile_q), f32),
                dma((W_SLOTS,)), dma((2,)),
            ] + [dma((n,))] * 12,
            compiler_params=pltpu.CompilerParams(collective_id=0, has_side_effects=True, vmem_limit_bytes=67043328),
        )
        out, k_new, v_new = call(x_rows, ln_gain[None, :], q_gain[None, :], k_gain[None, :], cos_tab, sin_tab,
                                 k_heads, v_heads, w_q, w_k, w_v, w_o)
        return out, jnp.transpose(k_new, (1, 0, 2)), jnp.transpose(v_new, (1, 0, 2))

    return jax.shard_map(device_step, mesh=mesh, in_specs=(row_spec, cache_spec, cache_spec, whole, whole, whole, whole, whole, whole, whole), out_specs=(row_spec, cache_spec, cache_spec), check_vma=False)
```

```python
import functools

import jax
import jax.numpy as jnp
from jax import lax
from jax.experimental import pallas as pl
from jax.experimental.pallas import tpu as pltpu
from jax.sharding import PartitionSpec as P

HEAD_DIM = 128
ROPE_THETA = 1.0e6
NORM_EPS = 1.0e-6
SCALE2 = HEAD_DIM ** -0.5 * 1.4426950408889634
KEY_BLOCK = 256
NEW_UNIT = 4
W_SLOTS = 3
W_COLS = 512
RELAY = 256
MESH = pl.DeviceIdType.MESH
NEG_INF = float('-inf')


def rope_tables(positions):
    half = HEAD_DIM // 2
    inv_freq = ROPE_THETA ** (-jnp.arange(half, dtype=jnp.float32) * (2.0 / HEAD_DIM))
    angles = positions.astype(jnp.float32)[:, None] * inv_freq[None, :]
    cos_tab = jnp.cos(angles)
    sin_tab = jnp.sin(angles)
    return jnp.concatenate([cos_tab, cos_tab], axis=-1), jnp.concatenate([-sin_tab, sin_tab], axis=-1)


def ring_order(n):
    chips = n // 2
    order = [(0, 0), (0, 1)]
    for d in range(1, chips // 2 + 1):
        if 2 * d == chips:
            order += [(d, 0), (d, 1)]
        else:
            order += [(d, 0), (chips - d, 0), (d, 1), (chips - d, 1)]
    return order


def make_kernel(n, rows, cache_rows, group):
    order = ring_order(n)
    chips = n // 2
    qcols = group * HEAD_DIM
    tile_q = 512
    halves = rows * group // tile_q
    tiles = n * halves
    phases = n // 2
    blocks = 2 * cache_rows // KEY_BLOCK
    per_chunk = cache_rows // KEY_BLOCK
    kv_per_tile = W_COLS // HEAD_DIM

    def kernel(x_ref, gain_ref, qg_ref, kg_ref, cos_ref, sin_ref, kc_raw, vc_raw, wq, wk, wv, wo,
               out_ref, kn_ref, vn_ref,
               h_ref, wbuf, kc, vc, kbuf, vbuf, qsend, qbuf, nkbuf, nvsend, nvbuf,
               s_ref, s2_ref, acc, m_ref, l_ref, mx_ref, mx2_ref, raw,
               wsem, rawsem, sk, rk, sv, rv, sq, rq, snk, rnk, snv, rnv, so, ro):
        me = lax.axis_index('cp')
        chip = me // 2
        core = me % 2

        def peer(j):
            if isinstance(j, int):
                dc, fl = order[j]
            else:
                dc, fl = jnp.int32(0), jnp.int32(0)
                for i, (a, b) in enumerate(order):
                    dc = jnp.where(j == i, a, dc)
                    fl = jnp.where(j == i, b, fl)
            return ((chip + dc) % chips) * 2 + (core + fl) % 2

        def remote(src, dst, ssem, rsem, dev):
            return pltpu.make_async_remote_copy(src_ref=src, dst_ref=dst, send_sem=ssem, recv_sem=rsem,
                                                device_id={'cp': dev}, device_id_type=MESH)

        def k_copy(dev, who):
            return remote(kc.at[dev], kbuf.at[who], sk.at[dev], rk.at[who], dev)

        def v_copy(dev, who):
            return remote(vc.at[dev], vbuf.at[who], sv.at[dev], rv.at[who], dev)

        def q_copy(dev, who):
            return remote(qsend.at[dev], qbuf.at[who], sq.at[dev], rq.at[who], dev)

        def nk_copy(dev, who):
            return remote(kn_ref.at[dev], nkbuf.at[who], snk.at[dev], rnk.at[who], dev)

        def nv_copy(dev, who):
            return remote(nvsend.at[dev], nvbuf.at[who], snv.at[dev], rnv.at[who], dev)

        def o_copy(dev, who):
            return remote(qsend.at[dev], h_ref.at[:, pl.ds(pl.multiple_of(who * qcols, qcols), qcols)],
                          so.at[dev], ro.at[who], dev)

        def w_copy(src, col, slot):
            return pltpu.make_async_copy(src.at[:, pl.ds(pl.multiple_of(col * W_COLS, W_COLS), W_COLS)],
                                         wbuf.at[slot], wsem.at[slot])

        def q_dest(t):
            if isinstance(t, int):
                return peer(t + 2 if t < n - 2 else n - 1 - t)
            return peer(jnp.where(t < n - 2, t + 2, n - 1 - t))

        for t in range(W_SLOTS):
            w_copy(wq, q_dest(t), t).start()
        def raw_copy(src, r, slot):
            return pltpu.make_async_copy(src.at[pl.ds(pl.multiple_of(r * RELAY, RELAY), RELAY)],
                                         raw.at[slot], rawsem.at[slot])

        relays = cache_rows // RELAY
        for r in range(2):
            raw_copy(kc_raw, r, r).start()

        barrier = pltpu.get_barrier_semaphore()
        for j in range(1, n):
            pl.semaphore_signal(barrier, inc=1, device_id={'cp': peer(j)}, device_id_type=MESH)
        pl.semaphore_wait(barrier, n - 1)

        def relay_k(r, _):
            slot = r % 2
            raw_copy(kc_raw, r, slot).wait()
            for i in range(RELAY // 64):
                to = pl.ds(pl.multiple_of(r * RELAY + i * 64, 64), 64)
                kc[:, to, :] = jnp.swapaxes(raw[slot, i * 64:(i + 1) * 64], 0, 1)

            @pl.when(r < relays - 2)
            def _():
                raw_copy(kc_raw, r + 2, slot).start()

            return 0

        lax.fori_loop(0, relays, relay_k, 0)
        for r in range(2):
            raw_copy(vc_raw, r, r).start()
        for j in range(1, n // 2):
            k_copy(peer(j), me).start()
        kbuf[me] = kc[me]

        gain = gain_ref[...].astype(jnp.float32)[None, :]

        def norm_rows(r, _):
            sl = pl.ds(pl.multiple_of(r * 32, 32), 32)
            xw = x_ref[sl, :].astype(jnp.float32)
            ms = jnp.mean(xw * xw, axis=-1, keepdims=True)
            h_ref[sl, :] = (xw * lax.rsqrt(ms + NORM_EPS) * gain).astype(jnp.bfloat16)
            return 0

        lax.fori_loop(0, rows // 32, norm_rows, 0)

        def init_tile(t, _):
            acc[t] = jnp.zeros((HEAD_DIM, tile_q), jnp.float32)
            m_ref[t] = jnp.full((8, tile_q), NEG_INF, jnp.float32)
            l_ref[t] = jnp.zeros((8, tile_q), jnp.float32)
            return 0

        lax.fori_loop(0, tiles, init_tile, 0)

        def project(slot):
            return jnp.dot(h_ref[...], wbuf[slot], preferred_element_type=jnp.float32).astype(jnp.bfloat16)

        def norm_rope(raw, head_gain):
            val = raw.astype(jnp.float32)
            ms = jnp.mean(val * val, axis=-1, keepdims=True)
            val = val * lax.rsqrt(ms + NORM_EPS) * head_gain
            return (val * cos_ref[...] + pltpu.roll(val, HEAD_DIM // 2, 1) * sin_ref[...]).astype(jnp.bfloat16)

        q_gain = qg_ref[...].astype(jnp.float32)
        k_gain = kg_ref[...].astype(jnp.float32)
        k_tiles = n // kv_per_tile

        def relay_v(r, rslot):
            for i in range(RELAY // 128):
                to = pl.ds(pl.multiple_of(r * RELAY + i * 128, 128), 128)
                heads = jnp.swapaxes(raw[rslot, i * 128:(i + 1) * 128], 0, 1)
                for g in range(n):
                    vc[g, :, to] = heads[g].T

        assert relays == n
        first_k, first_v, first_o = n, n + k_tiles, n + 2 * k_tiles

        def prefetch(i, lo, hi):
            slot = i % W_SLOTS
            if lo < first_k:
                @pl.when(i < first_k)
                def _():
                    w_copy(wq, q_dest(i), slot).start()

            for j in range(max(lo, first_k), min(hi, first_o)):
                @pl.when(i == j)
                def _(j=j):
                    src, first = (wk, first_k) if j < first_v else (wv, first_v)
                    w_copy(src, j - first, slot).start()

            if hi > first_o:
                @pl.when(jnp.logical_and(i >= first_o, i < first_o + n))
                def _():
                    w_copy(wo, i - first_o, slot).start()

        def q_tile(t, _):
            slot = t % W_SLOTS
            dest = q_dest(t)
            w_copy(wq, dest, slot).wait()
            rslot = t % 2
            raw_copy(vc_raw, t, rslot).wait()
            y = project(slot)
            relay_v(t, rslot)
            for g in range(group):
                cols = slice(g * HEAD_DIM, (g + 1) * HEAD_DIM)
                qsend[dest, :, cols] = norm_rope(y[:, cols], q_gain)

            @pl.when(t < relays - 2)
            def _():
                raw_copy(vc_raw, t + 2, rslot).start()

            prefetch(t + W_SLOTS, W_SLOTS, n + W_SLOTS)

            @pl.when(t < n - 1)
            def _():
                q_copy(dest, me).start()

            return 0

        lax.fori_loop(0, n, q_tile, 0)
        for j in range(1, n // 2):
            v_copy(peer(j), me).start()
        for j in range(n // 2, n - 2):
            k_copy(peer(j), me).start()
            v_copy(peer(j), me).start()
        qbuf[me] = qsend[me]
        vbuf[me] = vc[me]

        def k_tile(t, _):
            slot = (first_k + t) % W_SLOTS
            w_copy(wk, t, slot).wait()
            y = project(slot)
            for g in range(kv_per_tile):
                kn_ref[t * kv_per_tile + g] = norm_rope(y[:, g * HEAD_DIM:(g + 1) * HEAD_DIM], k_gain)
            prefetch(first_k + t + W_SLOTS, first_k + W_SLOTS, first_v + W_SLOTS)
            return 0

        lax.fori_loop(0, k_tiles, k_tile, 0)
        nkbuf[me] = kn_ref[me]

        def v_tile(t, _):
            slot = (first_v + t) % W_SLOTS
            w_copy(wv, t, slot).wait()
            y = project(slot)
            for g in range(kv_per_tile):
                val = y[:, g * HEAD_DIM:(g + 1) * HEAD_DIM]
                vn_ref[t * kv_per_tile + g] = val
                nvsend[t * kv_per_tile + g] = val.T
            prefetch(first_v + t + W_SLOTS, first_v + W_SLOTS, first_o + W_SLOTS)
            return 0

        lax.fori_loop(0, k_tiles, v_tile, 0)
        nvbuf[me] = nvsend[me]

        for j in range(1, n):
            nk_copy(peer(j), me).start()
            nv_copy(peer(j), me).start()
        for j in range(n - 2, n):
            k_copy(peer(j), me).start()
            v_copy(peer(j), me).start()

        def q_of(src, hf):
            per = tile_q // rows
            return jnp.concatenate(
                [qbuf[src, :, pl.ds(pl.multiple_of((hf * per + i) * HEAD_DIM, HEAD_DIM), HEAD_DIM)] for i in range(per)],
                axis=0)

        def qk(b, chunks, q):
            kk = kbuf[chunks[b // per_chunk], (b % per_chunk) * KEY_BLOCK:(b % per_chunk + 1) * KEY_BLOCK, :]
            s = lax.dot_general(kk, q, (((1,), (1,)), ((), ())), preferred_element_type=jnp.float32)
            s_ref[b * KEY_BLOCK:(b + 1) * KEY_BLOCK, :] = s
            return jnp.max(s.reshape(KEY_BLOCK // 8, 8, tile_q), axis=0)

        def fold(total, term, op):
            return term if total is None else op(total, term)

        def step(slot, chunks, next_chunks, next_q):
            m_old = m_ref[slot]
            m_new = jnp.maximum(m_old, jnp.max(mx_ref[...], axis=0, keepdims=True) * SCALE2)
            alpha = jnp.exp2(m_old - m_new)
            m_ref[slot] = m_new
            m_row = m_new[0:1]
            mx = ls = pv = None
            for b in range(blocks):
                p = jnp.exp2(s_ref[b * KEY_BLOCK:(b + 1) * KEY_BLOCK, :] * SCALE2 - m_row)
                ls = fold(ls, jnp.sum(p.reshape(KEY_BLOCK // 8, 8, tile_q), axis=0), jnp.add)
                mx = fold(mx, qk(b, next_chunks, next_q), jnp.maximum)
                vv = vbuf[chunks[b // per_chunk], :, (b % per_chunk) * KEY_BLOCK:(b % per_chunk + 1) * KEY_BLOCK]
                pv = fold(pv, jnp.dot(vv, p.astype(jnp.bfloat16), preferred_element_type=jnp.float32), jnp.add)
            mx_ref[...] = mx
            l_ref[slot] = l_ref[slot] * alpha + ls
            acc[slot] = acc[slot] * alpha[0:1] + pv

        pairs = [[peer(2 * p), peer(2 * p + 1)] for p in range(phases)]

        def block_of(p, t):
            i = t // halves
            return peer(n - 1 - i if p == phases - 1 else i)

        def block_after(p, t):
            if p == phases - 1:
                return block_of(p, jnp.minimum(t, tiles - 1))
            return jnp.where(t < tiles, block_of(p, jnp.minimum(t, tiles - 1)), block_of(p + 1, 0))

        def run_phase(p, after):
            def one(t, carry):
                src, nxt = carry
                if p < phases - 1:
                    @pl.when(t == tiles - 1)
                    def _():
                        for who in pairs[p + 1]:
                            k_copy(who, who).wait_recv()
                            v_copy(who, who).wait_recv()

                if p == 0:
                    @pl.when(jnp.logical_and((t + 1) % halves == 0, t < tiles - 1))
                    def _():
                        q_copy(nxt, nxt).wait_recv()

                later = pairs[min(p + 1, phases - 1)]
                next_chunks = [jnp.where(t == tiles - 1, b, a) for a, b in zip(pairs[p], later)]
                hf = t % halves
                step(src * halves + hf, pairs[p], next_chunks, q_of(nxt, (t + 1) % halves))
                after(t, src, hf)
                return nxt, block_after(p, t + 2)

            lax.fori_loop(0, tiles, one, (block_of(p, jnp.int32(0)), block_of(p, jnp.int32(1))))

        who = peer(1)
        k_copy(who, who).wait_recv()
        v_copy(who, who).wait_recv()
        first_q = q_of(me, 0)
        mx = None
        for b in range(blocks):
            mx = fold(mx, qk(b, [me, who], first_q), jnp.maximum)
        mx_ref[...] = mx

        for p in range(phases - 1):
            run_phase(p, lambda t, src, hf: None)

        for j in range(1, n):
            who = peer(j)
            nk_copy(who, who).wait_recv()
            nv_copy(who, who).wait_recv()

        new_steps = n + n - NEW_UNIT
        assert n == 2 * NEW_UNIT

        def new_place(k):
            unit = k // n
            return k - unit * (n - NEW_UNIT), unit

        def new_scores(src, unit, hf, b, q):
            lane = lax.broadcasted_iota(jnp.int32, (KEY_BLOCK, tile_q), 1)
            diff = lane % rows - lax.broadcasted_iota(jnp.int32, (KEY_BLOCK, tile_q), 0)
            kb = unit * NEW_UNIT + b
            s = lax.dot_general(nkbuf[kb], q, (((1,), (1,)), ((), ())), preferred_element_type=jnp.float32)
            s = jnp.where(diff >= (kb - src) * rows, s, NEG_INF)
            s2_ref[hf, b * KEY_BLOCK:(b + 1) * KEY_BLOCK, :] = s
            return jnp.max(s.reshape(KEY_BLOCK // 8, 8, tile_q), axis=0)

        def new_step(k, _):
            src, unit = new_place(k)
            src2, unit2 = new_place(jnp.minimum(k + 1, new_steps - 1))
            qs = [q_of(src2, hf) for hf in range(halves)]
            m_rows, alphas = [], []
            for hf in range(halves):
                m_old = m_ref[src * halves + hf]
                m_new = jnp.maximum(m_old, jnp.max(mx2_ref[hf], axis=0, keepdims=True) * SCALE2)
                alphas.append(jnp.exp2(m_old - m_new))
                m_ref[src * halves + hf] = m_new
                m_rows.append(m_new[0:1])
            mx, ls, pv = [None] * halves, [None] * halves, [None] * halves
            for b in range(NEW_UNIT):
                for hf in range(halves):
                    p = jnp.exp2(s2_ref[hf, b * KEY_BLOCK:(b + 1) * KEY_BLOCK, :] * SCALE2 - m_rows[hf])
                    ls[hf] = fold(ls[hf], jnp.sum(p.reshape(KEY_BLOCK // 8, 8, tile_q), axis=0), jnp.add)
                    mx[hf] = fold(mx[hf], new_scores(src2, unit2, hf, b, qs[hf]), jnp.maximum)
                    pv[hf] = fold(pv[hf], jnp.dot(nvbuf[unit * NEW_UNIT + b], p.astype(jnp.bfloat16),
                                                  preferred_element_type=jnp.float32), jnp.add)
            for hf in range(halves):
                slot = src * halves + hf
                mx2_ref[hf] = mx[hf]
                l_ref[slot] = l_ref[slot] * alphas[hf] + ls[hf]
                acc[slot] = acc[slot] * alphas[hf][0:1] + pv[hf]
            return 0

        for hf in range(halves):
            mx = None
            q = q_of(0, hf)
            for b in range(NEW_UNIT):
                mx = fold(mx, new_scores(0, 0, hf, b, q), jnp.maximum)
            mx2_ref[hf] = mx
        lax.fori_loop(0, new_steps, new_step, 0)

        for j in range(1, n):
            q_copy(peer(j), me).wait_send()

        def send_home(t, src, hf):
            slot = src * halves + hf
            o = acc[slot] / jnp.sum(l_ref[slot], axis=0, keepdims=True)
            o = o.T.astype(jnp.bfloat16)
            per = tile_q // rows
            for i in range(per):
                cols = pl.ds(pl.multiple_of((hf * per + i) * HEAD_DIM, HEAD_DIM), HEAD_DIM)
                qsend[src, :, cols] = o[i * rows:(i + 1) * rows]

            @pl.when(jnp.logical_and(hf == halves - 1, t < tiles - 1))
            def _():
                o_copy(src, me).start()

        run_phase(phases - 1, send_home)
        h_ref[:, pl.ds(pl.multiple_of(me * qcols, qcols), qcols)] = qsend[me]

        for j in range(n - 1, 0, -1):
            who = peer(j)
            o_copy(who, who).wait_recv()

        def out_tile(t, _):
            slot = (first_o + t) % W_SLOTS
            w_copy(wo, t, slot).wait()
            y = jnp.dot(h_ref[...], wbuf[slot], preferred_element_type=jnp.float32)
            cols = pl.ds(pl.multiple_of(t * W_COLS, W_COLS), W_COLS)
            out_ref[:, cols] = (x_ref[:, cols].astype(jnp.float32) + y).astype(jnp.bfloat16)
            prefetch(first_o + t + W_SLOTS, first_o + W_SLOTS, first_o + n + W_SLOTS)
            return 0

        lax.fori_loop(0, n, out_tile, 0)

        for j in range(1, n):
            who = peer(j)
            for copy in (k_copy, v_copy, nk_copy, nv_copy, o_copy):
                copy(who, me).wait_send()

    return kernel


def finish(out_in, k_in, v_in, out_ref, k_ref, v_ref, rows_buf, heads_buf, turned_buf, isem, osem):
    parts = rows_buf.shape[0]
    part = rows_buf.shape[1]
    rows_in = [pltpu.make_async_copy(out_in.at[pl.ds(i * part, part)], rows_buf.at[i], isem.at[i]) for i in range(parts)]
    rows_out = [pltpu.make_async_copy(rows_buf.at[i], out_ref.at[pl.ds(i * part, part)], osem.at[i]) for i in range(parts)]
    heads_in = [pltpu.make_async_copy(src, heads_buf.at[i], isem.at[parts + i]) for i, src in enumerate((k_in, v_in))]
    turned_out = [pltpu.make_async_copy(turned_buf.at[i], dst, osem.at[parts + i]) for i, dst in enumerate((k_ref, v_ref))]
    for copy in heads_in + rows_in:
        copy.start()
    for i in range(2):
        heads_in[i].wait()
        for r in range(0, turned_buf.shape[1], 64):
            turned_buf[i, r:r + 64] = jnp.swapaxes(heads_buf[i, :, r:r + 64], 0, 1)
        turned_out[i].start()
    for i in range(parts):
        rows_in[i].wait()
        rows_out[i].start()
    for copy in turned_out + rows_out:
        copy.wait()


def solution(mesh):
    n = mesh.shape['cp']
    row_spec = P(('dp', 'cp'), None)
    cache_spec = P(('dp', 'cp'), None, None)
    whole = P()

    def device_step(x_rows, k_cache, v_cache, ln_gain, w_q, w_k, w_v, w_o, q_gain, k_gain):
        rows, hidden = x_rows.shape
        cache_rows, kv_heads, _ = k_cache.shape
        group = w_q.shape[1] // HEAD_DIM // kv_heads
        q_rows = rows * group
        tile_q = 512
        tiles = n * q_rows // tile_q
        positions = cache_rows * n + lax.axis_index('cp') * rows + jnp.arange(rows)
        cos_tab, sin_tab = rope_tables(positions)
        bf16 = jnp.bfloat16
        f32 = jnp.float32
        vmem = pl.BlockSpec(memory_space=pltpu.VMEM)
        hbm = pl.BlockSpec(memory_space=pl.ANY)
        dma = pltpu.SemaphoreType.DMA
        call = pl.pallas_call(
            make_kernel(n, rows, cache_rows, group),
            out_shape=(jax.ShapeDtypeStruct((rows, hidden), bf16),
                       jax.ShapeDtypeStruct((kv_heads, rows, HEAD_DIM), bf16),
                       jax.ShapeDtypeStruct((kv_heads, rows, HEAD_DIM), bf16)),
            in_specs=[vmem] * 6 + [hbm] * 6,
            out_specs=[vmem] * 3,
            scratch_shapes=[
                pltpu.VMEM((rows, hidden), bf16),
                pltpu.VMEM((W_SLOTS, hidden, W_COLS), bf16),
                pltpu.VMEM((n, cache_rows, HEAD_DIM), bf16),
                pltpu.VMEM((n, HEAD_DIM, cache_rows), bf16),
                pltpu.VMEM((n, cache_rows, HEAD_DIM), bf16),
                pltpu.VMEM((n, HEAD_DIM, cache_rows), bf16),
                pltpu.VMEM((n, rows, group * HEAD_DIM), bf16),
                pltpu.VMEM((n, rows, group * HEAD_DIM), bf16),
                pltpu.VMEM((n, rows, HEAD_DIM), bf16),
                pltpu.VMEM((n, HEAD_DIM, rows), bf16),
                pltpu.VMEM((n, HEAD_DIM, rows), bf16),
                pltpu.VMEM((2 * cache_rows, tile_q), f32),
                pltpu.VMEM((q_rows // tile_q, NEW_UNIT * KEY_BLOCK, tile_q), f32),
                pltpu.VMEM((tiles, HEAD_DIM, tile_q), f32),
                pltpu.VMEM((tiles, 8, tile_q), f32),
                pltpu.VMEM((tiles, 8, tile_q), f32),
                pltpu.VMEM((8, tile_q), f32),
                pltpu.VMEM((q_rows // tile_q, 8, tile_q), f32),
                pltpu.VMEM((2, RELAY, kv_heads, HEAD_DIM), bf16),
                dma((W_SLOTS,)), dma((2,)),
            ] + [dma((n,))] * 12,
            compiler_params=pltpu.CompilerParams(collective_id=0, has_side_effects=True, vmem_limit_bytes=67043328),
        )
        out, k_new, v_new = call(x_rows, ln_gain, q_gain[None, :], k_gain[None, :], cos_tab, sin_tab,
                                 k_cache, v_cache, w_q, w_k, w_v, w_o)
        parts = 4
        return pl.pallas_call(
            finish,
            out_shape=(jax.ShapeDtypeStruct((rows, hidden), bf16),
                       jax.ShapeDtypeStruct((rows, kv_heads, HEAD_DIM), bf16),
                       jax.ShapeDtypeStruct((rows, kv_heads, HEAD_DIM), bf16)),
            in_specs=[hbm] * 3,
            out_specs=[hbm] * 3,
            scratch_shapes=[pltpu.VMEM((parts, rows // parts, hidden), bf16),
                            pltpu.VMEM((2, kv_heads, rows, HEAD_DIM), bf16),
                            pltpu.VMEM((2, rows, kv_heads, HEAD_DIM), bf16),
                            dma((parts + 2,)), dma((parts + 2,))],
        )(out, k_new, v_new)

    return jax.shard_map(device_step, mesh=mesh, in_specs=(row_spec, cache_spec, cache_spec, whole, whole, whole, whole, whole, whole, whole), out_specs=(row_spec, cache_spec, cache_spec), check_vma=False)
```
